512 devices in a mesh: freq: 16 (over y, z_hi, core), stn: 32 (over x, z_lo).
Axes of the slice: x: 4, y: 4, z: 16 (z_hi: 2, z_lo: 8; z = z_hi * 8 + z_lo), core: 2. Of those that a mesh axis runs over, the one named last changes fastest.
Arguments:
- samples: bfloat16 [16, 1024, 24, 2, 128], P('freq', 'stn'), may hold values from -8 to 8, as said below
- window: float32 [128], replicated, may hold values from 0.1 to 1
- group_of_device: int32 [32], replicated, may hold values from 0 to 31, each once
- owner_map: int32 [32, 32], replicated, may hold values from 0 to 31, as said below
Outputs:
- owned: bfloat16 [2, 128, 32, 32, 1024], P(None, None, 'stn', 'freq')
The draws below stay inside these ranges and needn't reach their ends.
Inputs may be any that keep to these rules, and one draw needn't show every extreme that they name: `samples`: samples are finite and bounded. Every row and every column of owner_map names each stn index exactly once.
All inputs are finite; a program needn't handle non-finite values.
Results may differ from the reference program's by a relative error of at most 0.0065.
Values may be sent and summed in bfloat16 or wider, within the bound.
A program may use at most 64 MiB of HBM per device.

```python
import math
import jax
import jax.numpy as jnp
from jax import lax

FFT_LEN = 128
AVG = 16
SPEC = 24
GRP_IN = 32
CH_OUT = 8
GROUPS = 32
BANDS = 16
INPUTS = 1024
CHANNELS = 128


def draw_samples(key, part):
    sky_sources = 32
    keys = jax.random.split(key, 3)
    shape = (BANDS, INPUTS, SPEC, 2, FFT_LEN)
    gains = jax.random.normal(keys[1], (INPUTS, sky_sources), jnp.float32)
    signals = jax.random.normal(keys[2], (BANDS, sky_sources, SPEC, 2, FFT_LEN), jnp.float32)
    common = jnp.einsum('ik,bktrn->bitrn', gains, signals) / math.sqrt(sky_sources)
    noise = jax.random.normal(keys[0], shape, jnp.float32)
    total = 0.55 * noise + common
    return jnp.clip(total, -8.0, 8.0).astype(jnp.bfloat16)


def draw_owner_map(key, part):
    keys = jax.random.split(key, 3)
    row_shift = jax.random.permutation(keys[0], GROUPS)
    col_shift = jax.random.permutation(keys[1], GROUPS)
    labels = jax.random.permutation(keys[2], GROUPS)
    return labels[(row_shift[:, None] + col_shift[None, :]) % GROUPS].astype(jnp.int32)


def setup_inputs(seed: int = 0) -> dict:
    key_of = jax.random.split(jax.random.key(seed), 5)
    return {
        "samples": draw_samples(jax.random.fold_in(key_of[4], 71), 0),
        "window": jnp.clip(jnp.exp(jax.random.uniform(key_of[1], (FFT_LEN,), jnp.float32, math.log(0.1), math.log(1.0))), 0.1, 1.0),
        "group_of_device": jax.random.permutation(key_of[2], GROUPS).astype(jnp.int32),
        "owner_map": draw_owner_map(jax.random.fold_in(key_of[4], 71), 0),
    }


def channel_matrix(window):
    length = window.shape[0]
    index = jnp.arange(length, dtype=jnp.int32)
    product = index[:, None] * index[None, :] % length
    theta = product.astype(jnp.float32) * (2.0 * math.pi / length)
    weights = window[:, None] / math.sqrt(length)
    cosine = weights * jnp.cos(theta)
    sine = weights * jnp.sin(theta)
    upper = jnp.concatenate([cosine, -sine], axis=1)
    lower = jnp.concatenate([sine, cosine], axis=1)
    return jnp.concatenate([upper, lower], axis=0)

def split_matrix(matrix):
    high = matrix.astype(jnp.bfloat16)
    low = (matrix - high.astype(jnp.float32)).astype(jnp.bfloat16)
    return (high, low)

def channelize(block, high, low):
    rows = block.shape[0]
    flat = block.reshape(rows * SPEC, 2 * FFT_LEN)
    spectra = jnp.dot(flat, high, preferred_element_type=jnp.float32) + jnp.dot(flat, low, preferred_element_type=jnp.float32)
    spectra = spectra.astype(jnp.bfloat16).reshape(rows, SPEC, 2, CH_OUT, AVG)
    return spectra.transpose(3, 0, 2, 1, 4).reshape(CH_OUT, rows, 2 * SPEC * AVG)

def reference(samples, window, group_of_device, owner_map):
    high, low = split_matrix(channel_matrix(window))
    order = jnp.arange(GROUPS, dtype=jnp.int32)
    dev_of_group = jnp.zeros((GROUPS,), jnp.int32).at[group_of_device].set(order)
    grouped = samples.reshape(BANDS, GROUPS, GRP_IN, SPEC, 2, FFT_LEN)
    grouped = jnp.take(grouped, dev_of_group, axis=1).reshape(BANDS, INPUTS, SPEC, 2, FFT_LEN)
    column_for = jnp.zeros((GROUPS, GROUPS), jnp.int32).at[order[:, None], owner_map].set(jnp.broadcast_to(order[None, :], (GROUPS, GROUPS)))

    def one_band(band):
        spectra = channelize(band, high, low).astype(jnp.float32)
        half = spectra.shape[2] // 2
        swapped = jnp.concatenate([spectra[..., half:], -spectra[..., :half]], axis=-1)
        stacked = jnp.stack([spectra, swapped])
        vis = jnp.einsum('pcak,cbk->pcab', stacked, spectra)
        vis = (vis * (1.0 / (AVG * SPEC))).astype(jnp.bfloat16)
        vis = vis.reshape(2, CH_OUT, GROUPS, GRP_IN, GROUPS, GRP_IN).transpose(0, 1, 2, 4, 3, 5)
        vis = vis.reshape(2, CH_OUT, GROUPS, GROUPS, GRP_IN * GRP_IN)
        picked = jnp.take_along_axis(vis, column_for[None, None, :, :, None], axis=3)
        return picked.transpose(0, 1, 3, 2, 4)
    result = lax.map(one_band, grouped)
    result = result.transpose(1, 0, 2, 3, 4, 5)
    return result.reshape(2, CHANNELS, GROUPS, GROUPS, GRP_IN * GRP_IN)
```

```python
import math

import jax
import jax.numpy as jnp
import numpy as np
from jax import lax
from jax.experimental import pallas as pl
from jax.experimental.pallas import tpu as pltpu
from jax.sharding import PartitionSpec as P

FFT_LEN = 128
AVG = 16
SPEC = 24
CH_OUT = 8
ROWS = 32
DEPTH = 2 * SPEC * AVG
NX = 4
NZ = 8
NF = 16
STN = NX * NZ
MESH = pl.DeviceIdType.MESH


def dft_table():
    index = np.arange(FFT_LEN)
    theta = (index[:, None] * index[None, :] % FFT_LEN) * (2.0 * math.pi / FFT_LEN)
    table = np.concatenate([np.cos(theta), np.sin(theta)], axis=1) / math.sqrt(FFT_LEN)
    return table.astype(np.float32)


def swap_blocks(blocks, width, lane):
    blocks = list(blocks)
    step = 1
    while step < len(blocks):
        low = (lane // (width * step)) % 2 == 0
        shift = width * step
        for i in range(len(blocks)):
            if i & step:
                continue
            a, b = blocks[i], blocks[i | step]
            blocks[i] = jnp.where(low, a, pltpu.roll(b, shift, 1))
            blocks[i | step] = jnp.where(low, pltpu.roll(a, 128 - shift, 1), b)
        step *= 2
    return blocks


def kernel(
    rows_tab, cols_tab, samples, taps, out,
    uc, us, chan, held, mixed, pairs, outgoing,
    in_send, in_recv, out_send, out_recv, own_sem,
):
    f = lax.axis_index("freq")
    s = lax.axis_index("stn")
    x = s // NZ
    zl = s % NZ

    high = taps[...].astype(jnp.bfloat16)
    low = (taps[...] - high.astype(jnp.float32)).astype(jnp.bfloat16)
    both = jnp.concatenate([high, low], axis=0)
    chunk = 256

    @pl.loop(0, 2 * ROWS * SPEC // chunk)
    def _(i):
        rows = pl.ds(pl.multiple_of(i * chunk, chunk), chunk)
        block = samples[rows, :]
        full = jnp.dot(
            jnp.concatenate([block, block], axis=1), both, preferred_element_type=jnp.float32
        )
        uc[rows, :] = full[:, :FFT_LEN]
        us[rows, :] = full[:, FFT_LEN:]

    lane = lax.broadcasted_iota(jnp.int32, (ROWS, 128), 1)
    for t8 in range(SPEC // 8):
        for part in range(2):
            blocks = []
            for t in range(8):
                at = 2 * (t8 * 8 + t)
                re = pl.ds(at, ROWS, stride=2 * SPEC)
                im = pl.ds(at + 1, ROWS, stride=2 * SPEC)
                if part == 0:
                    blocks.append(uc[re, :] + us[im, :])
                else:
                    blocks.append(uc[im, :] - us[re, :])
            blocks = swap_blocks(blocks, AVG, lane)
            for k in range(CH_OUT):
                start = (2 * t8 + part) * 128
                chan[k, :, start : start + 128] = blocks[k].astype(jnp.bfloat16)
    held[s] = chan[zl]

    def block_to(src, at, to_x, to_z):
        return pltpu.make_async_remote_copy(
            src_ref=src,
            dst_ref=held.at[at],
            send_sem=in_send,
            recv_sem=in_recv.at[at],
            device_id=(f, to_x * NZ + to_z),
            device_id_type=MESH,
        )

    def along_x(src, at):
        for dx in (1, 3, 2):
            block_to(src, at, (x + dx) % NX, zl).start()

    steps = (1, 7, 2, 6, 3, 5, 4)
    for dz in steps:
        to = (zl + dz) % NZ
        block_to(chan.at[to], s, x, to).start()
    along_x(chan.at[zl], s)
    for dz in steps:
        at = x * NZ + (zl - dz + NZ) % NZ
        block_to(held.at[at], at, (x + 1) % NX, zl).wait_recv()
        along_x(held.at[at], at)
    for dx in (1, 3, 2):
        for z in range(NZ):
            at = ((x + dx) % NX) * NZ + z
            block_to(held.at[at], at, (x + 1) % NX, zl).wait_recv()

    lane8 = lax.broadcasted_iota(jnp.int32, (8, 128), 1)
    channel = f * CH_OUT + zl

    @pl.loop(0, NF)
    def _(i):
        p = (f + i) % NF
        for r in range(2):
            g1 = 2 * p + r
            a = held[rows_tab[g1]]
            turned = []
            for t8 in range(SPEC // 8):
                turned.append(a[:, (2 * t8 + 1) * 128 : (2 * t8 + 2) * 128])
                turned.append(-a[:, 2 * t8 * 128 : (2 * t8 + 1) * 128])
            left = jnp.concatenate([a, jnp.concatenate(turned, axis=1)], axis=0)
            right = jnp.concatenate(
                [held[cols_tab[g1, x * NZ + oz]] for oz in range(NZ)], axis=0
            )
            vis = lax.dot_general(
                left, right, (((1,), (1,)), ((), ())), preferred_element_type=jnp.float32
            ) * (1.0 / (AVG * SPEC))
            for h in range(2):
                mixed[r, h] = vis[:, h * 128 : (h + 1) * 128]
                for part in range(2):
                    blocks = [
                        mixed[r, h, pl.ds(part * ROWS + j, 8, stride=4), :] for j in range(4)
                    ]
                    blocks = swap_blocks(blocks, ROWS, lane8)
                    for q in range(4):
                        pairs[4 * h + q, part, pl.ds(r, 8, stride=2), :] = blocks[q]
        outgoing[i] = pairs[...].astype(jnp.bfloat16)
        for oz in range(NZ):
            mine = jnp.logical_and(i == 0, zl == oz)

            @pl.when(jnp.logical_not(mine))
            def _():
                pltpu.make_async_remote_copy(
                    src_ref=outgoing.at[i, oz],
                    dst_ref=out.at[:, channel],
                    send_sem=out_send,
                    recv_sem=out_recv,
                    device_id=(p, x * NZ + oz),
                    device_id_type=MESH,
                ).start()

            @pl.when(mine)
            def _():
                pltpu.make_async_copy(
                    outgoing.at[0, oz], out.at[:, channel], own_sem
                ).start()

    pltpu.make_async_copy(outgoing.at[0, 0], out.at[:, channel], own_sem).wait()
    rest = pltpu.make_async_remote_copy(
        src_ref=out.at[:, pl.ds(0, NF * NZ - 1)],
        dst_ref=out.at[:, pl.ds(0, NF * NZ - 1)],
        send_sem=out_send,
        recv_sem=out_recv,
        device_id=(f, x * NZ + (zl + 1) % NZ),
        device_id_type=MESH,
    )
    rest.wait_send()
    rest.wait_recv()
    sent = pltpu.make_async_remote_copy(
        src_ref=held.at[pl.ds(0, STN - 1)],
        dst_ref=held.at[pl.ds(0, STN - 1)],
        send_sem=in_send,
        recv_sem=in_recv.at[0],
        device_id=(f, x * NZ + (zl + 1) % NZ),
        device_id_type=MESH,
    )
    sent.wait_send()


def shards(samples, window, group_of_device, owner_map):
    order = jnp.arange(STN, dtype=jnp.int32)
    at_group = group_of_device[None, :] == order[:, None]
    rows_tab = jnp.sum(jnp.where(at_group, order[None, :], 0), axis=1)
    hit = owner_map[:, :, None] == order[None, None, :]
    cols_tab = jnp.sum(jnp.where(hit, rows_tab[None, :, None], 0), axis=1)
    taps = window[:, None] * jnp.asarray(dft_table())
    flat = samples.reshape(2 * ROWS * SPEC, FFT_LEN)
    smem = pl.BlockSpec(memory_space=pltpu.SMEM)
    vmem = pl.BlockSpec(memory_space=pltpu.VMEM)
    got = pl.pallas_call(
        kernel,
        out_shape=jax.ShapeDtypeStruct((2, NF * CH_OUT, 16, 128), jnp.bfloat16),
        in_specs=[smem, smem, vmem, vmem],
        out_specs=pl.BlockSpec(memory_space=pl.ANY),
        scratch_shapes=[
            pltpu.VMEM((2 * ROWS * SPEC, FFT_LEN), jnp.float32),
            pltpu.VMEM((2 * ROWS * SPEC, FFT_LEN), jnp.float32),
            pltpu.VMEM((CH_OUT, ROWS, DEPTH), jnp.bfloat16),
            pltpu.VMEM((STN, ROWS, DEPTH), jnp.bfloat16),
            pltpu.VMEM((2, 2, 2 * ROWS, 128), jnp.float32),
            pltpu.VMEM((NZ, 2, 16, 128), jnp.float32),
            pltpu.VMEM((NF, NZ, 2, 16, 128), jnp.bfloat16),
            pltpu.SemaphoreType.DMA,
            pltpu.SemaphoreType.DMA((STN,)),
            pltpu.SemaphoreType.DMA,
            pltpu.SemaphoreType.DMA,
            pltpu.SemaphoreType.DMA,
        ],
        compiler_params=pltpu.CompilerParams(
            has_side_effects=True, vmem_limit_bytes=32 * 1024 * 1024
        ),
        name="correlate_and_regroup",
    )(rows_tab, cols_tab, flat, taps)
    got = got.reshape(2, NF * CH_OUT, 8, 2, 128).transpose(0, 1, 3, 2, 4)
    return got.reshape(2, NF * CH_OUT, 1, 2, ROWS * ROWS)


def solution(mesh):
    return jax.shard_map(
        shards,
        mesh=mesh,
        in_specs=(P("freq", "stn", None, None, None), P(), P(), P()),
        out_specs=P(None, None, "stn", "freq", None),
        check_vma=False,
    )
```

```python
import math

import jax
import jax.numpy as jnp
import numpy as np
from jax import lax
from jax.experimental import pallas as pl
from jax.experimental.pallas import tpu as pltpu
from jax.sharding import PartitionSpec as P

FFT_LEN = 128
AVG = 16
SPEC = 24
CH_OUT = 8
ROWS = 32
DEPTH = 2 * SPEC * AVG
NX = 4
NZ = 8
NF = 16
STN = NX * NZ
MESH = pl.DeviceIdType.MESH


def dft_table():
    index = np.arange(FFT_LEN)
    theta = (index[:, None] * index[None, :] % FFT_LEN) * (2.0 * math.pi / FFT_LEN)
    table = np.concatenate([np.cos(theta), np.sin(theta)], axis=1) / math.sqrt(FFT_LEN)
    return table.astype(np.float32)


def swap_blocks(blocks, width, lane):
    blocks = list(blocks)
    step = 1
    while step < len(blocks):
        low = (lane // (width * step)) % 2 == 0
        shift = width * step
        for i in range(len(blocks)):
            if i & step:
                continue
            a, b = blocks[i], blocks[i | step]
            blocks[i] = jnp.where(low, a, pltpu.roll(b, shift, 1))
            blocks[i | step] = jnp.where(low, pltpu.roll(a, 128 - shift, 1), b)
        step *= 2
    return blocks


def kernel(
    rows_tab, cols_tab, samples, taps, out,
    uc, us, chan, held, mixed, pairs, outgoing,
    in_send, in_recv, out_send, out_recv, own_sem,
):
    f = lax.axis_index("freq")
    s = lax.axis_index("stn")
    x = s // NZ
    zl = s % NZ

    barrier = pltpu.get_barrier_semaphore()

    def greet(to_f, to_s):
        pl.semaphore_signal(barrier, inc=1, device_id=(to_f, to_s), device_id_type=MESH)

    for d in range(1, NZ):
        greet(f, x * NZ + (zl + d) % NZ)
    for d in range(1, NX):
        greet(f, ((x + d) % NX) * NZ + zl)
    for d in range(1, NF):
        greet((f + d) % NF, s)

    high = taps[...].astype(jnp.bfloat16)
    low = (taps[...] - high.astype(jnp.float32)).astype(jnp.bfloat16)
    both = jnp.concatenate([high, low], axis=0)
    chunk = 256

    @pl.loop(0, 2 * ROWS * SPEC // chunk)
    def _(i):
        rows = pl.ds(pl.multiple_of(i * chunk, chunk), chunk)
        block = samples[rows, :]
        full = jnp.dot(
            jnp.concatenate([block, block], axis=1), both, preferred_element_type=jnp.float32
        )
        uc[rows, :] = full[:, :FFT_LEN]
        us[rows, :] = full[:, FFT_LEN:]

    lane = lax.broadcasted_iota(jnp.int32, (ROWS, 128), 1)
    for t8 in range(SPEC // 8):
        for part in range(2):
            blocks = []
            for t in range(8):
                at = 2 * (t8 * 8 + t)
                re = pl.ds(at, ROWS, stride=2 * SPEC)
                im = pl.ds(at + 1, ROWS, stride=2 * SPEC)
                if part == 0:
                    blocks.append(uc[re, :] + us[im, :])
                else:
                    blocks.append(uc[im, :] - us[re, :])
            blocks = swap_blocks(blocks, AVG, lane)
            for k in range(CH_OUT):
                start = (2 * t8 + part) * 128
                chan[k, :, start : start + 128] = blocks[k].astype(jnp.bfloat16)
    held[s] = chan[zl]
    pl.semaphore_wait(barrier, NZ + NX + NF - 3)

    def block_to(src, at, to_x, to_z):
        return pltpu.make_async_remote_copy(
            src_ref=src,
            dst_ref=held.at[at],
            send_sem=in_send,
            recv_sem=in_recv.at[at],
            device_id=(f, to_x * NZ + to_z),
            device_id_type=MESH,
        )

    def along_x(src, at):
        for dx in (1, 3, 2):
            block_to(src, at, (x + dx) % NX, zl).start()

    steps = (1, 7, 2, 6, 3, 5, 4)
    for dz in steps:
        to = (zl + dz) % NZ
        block_to(chan.at[to], s, x, to).start()
    along_x(chan.at[zl], s)
    for dz in steps:
        at = x * NZ + (zl - dz + NZ) % NZ
        block_to(held.at[at], at, (x + 1) % NX, zl).wait_recv()
        along_x(held.at[at], at)
    for dx in (1, 3, 2):
        for z in range(NZ):
            at = ((x + dx) % NX) * NZ + z
            block_to(held.at[at], at, (x + 1) % NX, zl).wait_recv()

    lane8 = lax.broadcasted_iota(jnp.int32, (8, 128), 1)
    channel = f * CH_OUT + zl

    @pl.loop(0, NF)
    def _(i):
        p = (f + i) % NF
        for r in range(2):
            g1 = 2 * p + r
            a = held[rows_tab[g1]]
            turned = []
            for t8 in range(SPEC // 8):
                turned.append(a[:, (2 * t8 + 1) * 128 : (2 * t8 + 2) * 128])
                turned.append(-a[:, 2 * t8 * 128 : (2 * t8 + 1) * 128])
            left = jnp.concatenate([a, jnp.concatenate(turned, axis=1)], axis=0)
            right = jnp.concatenate(
                [held[cols_tab[g1, x * NZ + oz]] for oz in range(NZ)], axis=0
            )
            vis = lax.dot_general(
                left, right, (((1,), (1,)), ((), ())), preferred_element_type=jnp.float32
            ) * (1.0 / (AVG * SPEC))
            for h in range(2):
                mixed[r, h] = vis[:, h * 128 : (h + 1) * 128]
                for part in range(2):
                    blocks = [
                        mixed[r, h, pl.ds(part * ROWS + j, 8, stride=4), :] for j in range(4)
                    ]
                    blocks = swap_blocks(blocks, ROWS, lane8)
                    for q in range(4):
                        pairs[4 * h + q, part, pl.ds(r, 8, stride=2), :] = blocks[q]
        outgoing[i] = pairs[...].astype(jnp.bfloat16)
        for oz in range(NZ):
            mine = jnp.logical_and(i == 0, zl == oz)

            @pl.when(jnp.logical_not(mine))
            def _():
                pltpu.make_async_remote_copy(
                    src_ref=outgoing.at[i, oz],
                    dst_ref=out.at[:, channel],
                    send_sem=out_send,
                    recv_sem=out_recv,
                    device_id=(p, x * NZ + oz),
                    device_id_type=MESH,
                ).start()

            @pl.when(mine)
            def _():
                pltpu.make_async_copy(
                    outgoing.at[0, oz], out.at[:, channel], own_sem
                ).start()

    pltpu.make_async_copy(outgoing.at[0, 0], out.at[:, channel], own_sem).wait()
    rest = pltpu.make_async_remote_copy(
        src_ref=out.at[:, pl.ds(0, NF * NZ - 1)],
        dst_ref=out.at[:, pl.ds(0, NF * NZ - 1)],
        send_sem=out_send,
        recv_sem=out_recv,
        device_id=(f, x * NZ + (zl + 1) % NZ),
        device_id_type=MESH,
    )
    rest.wait_send()
    rest.wait_recv()
    sent = pltpu.make_async_remote_copy(
        src_ref=held.at[pl.ds(0, STN - 1)],
        dst_ref=held.at[pl.ds(0, STN - 1)],
        send_sem=in_send,
        recv_sem=in_recv.at[0],
        device_id=(f, x * NZ + (zl + 1) % NZ),
        device_id_type=MESH,
    )
    sent.wait_send()


def shards(samples, window, group_of_device, owner_map):
    order = jnp.arange(STN, dtype=jnp.int32)
    at_group = group_of_device[None, :] == order[:, None]
    rows_tab = jnp.sum(jnp.where(at_group, order[None, :], 0), axis=1)
    hit = owner_map[:, :, None] == order[None, None, :]
    cols_tab = jnp.sum(jnp.where(hit, rows_tab[None, :, None], 0), axis=1)
    taps = window[:, None] * jnp.asarray(dft_table())
    flat = samples.reshape(2 * ROWS * SPEC, FFT_LEN)
    smem = pl.BlockSpec(memory_space=pltpu.SMEM)
    vmem = pl.BlockSpec(memory_space=pltpu.VMEM)
    got = pl.pallas_call(
        kernel,
        out_shape=jax.ShapeDtypeStruct((2, NF * CH_OUT, 16, 128), jnp.bfloat16),
        in_specs=[smem, smem, vmem, vmem],
        out_specs=pl.BlockSpec(memory_space=pl.ANY),
        scratch_shapes=[
            pltpu.VMEM((2 * ROWS * SPEC, FFT_LEN), jnp.float32),
            pltpu.VMEM((2 * ROWS * SPEC, FFT_LEN), jnp.float32),
            pltpu.VMEM((CH_OUT, ROWS, DEPTH), jnp.bfloat16),
            pltpu.VMEM((STN, ROWS, DEPTH), jnp.bfloat16),
            pltpu.VMEM((2, 2, 2 * ROWS, 128), jnp.float32),
            pltpu.VMEM((NZ, 2, 16, 128), jnp.float32),
            pltpu.VMEM((NF, NZ, 2, 16, 128), jnp.bfloat16),
            pltpu.SemaphoreType.DMA,
            pltpu.SemaphoreType.DMA((STN,)),
            pltpu.SemaphoreType.DMA,
            pltpu.SemaphoreType.DMA,
            pltpu.SemaphoreType.DMA,
        ],
        compiler_params=pltpu.CompilerParams(
            has_side_effects=True, collective_id=0, vmem_limit_bytes=32 * 1024 * 1024
        ),
        name="correlate_and_regroup",
    )(rows_tab, cols_tab, flat, taps)
    got = got.reshape(2, NF * CH_OUT, 8, 2, 128).transpose(0, 1, 3, 2, 4)
    return got.reshape(2, NF * CH_OUT, 1, 2, ROWS * ROWS)


def solution(mesh):
    return jax.shard_map(
        shards,
        mesh=mesh,
        in_specs=(P("freq", "stn", None, None, None), P(), P(), P()),
        out_specs=P(None, None, "stn", "freq", None),
        check_vma=False,
    )
```

```python
import math

import jax
import jax.numpy as jnp
import numpy as np
from jax import lax
from jax.experimental import pallas as pl
from jax.experimental.pallas import tpu as pltpu
from jax.sharding import PartitionSpec as P

FFT_LEN = 128
AVG = 16
SPEC = 24
CH_OUT = 8
ROWS = 32
DEPTH = 2 * SPEC * AVG
NX = 4
NZ = 8
NF = 16
STN = NX * NZ
MESH = pl.DeviceIdType.MESH


def dft_table():
    index = np.arange(FFT_LEN)
    theta = (index[:, None] * index[None, :] % FFT_LEN) * (2.0 * math.pi / FFT_LEN)
    table = np.concatenate([np.cos(theta), np.sin(theta)], axis=1) / math.sqrt(FFT_LEN)
    return table.astype(np.float32)


def swap_blocks(blocks, width, lane):
    blocks = list(blocks)
    step = 1
    while step < len(blocks):
        low = (lane // (width * step)) % 2 == 0
        shift = width * step
        for i in range(len(blocks)):
            if i & step:
                continue
            a, b = blocks[i], blocks[i | step]
            blocks[i] = jnp.where(low, a, pltpu.roll(b, shift, 1))
            blocks[i | step] = jnp.where(low, pltpu.roll(a, 128 - shift, 1), b)
        step *= 2
    return blocks


def column(row, size):
    lane = lax.broadcasted_iota(jnp.int32, (size, size), 1)
    sub = lax.broadcasted_iota(jnp.int32, (size, size), 0)
    return jnp.sum(jnp.where(lane == sub, row, jnp.zeros_like(row)), axis=1, keepdims=True)


def kernel(
    samples_hbm, window_hbm, groups_hbm, owners_hbm, table_hbm, out,
    samples, window, groups, owners, table, tab_vmem, tab,
    uc, us, chan, held, mixed, pairs, outgoing,
    load_sem, chunk_sem, in_send, in_recv, out_send, out_recv, own_sem,
):
    f = lax.axis_index("freq")
    s = lax.axis_index("stn")
    x = s // NZ
    zl = s % NZ

    barrier = pltpu.get_barrier_semaphore()

    def greet(to_f, to_s):
        pl.semaphore_signal(barrier, inc=1, device_id=(to_f, to_s), device_id_type=MESH)

    for d in range(1, NZ):
        greet(f, x * NZ + (zl + d) % NZ)
    for d in range(1, NX):
        greet(f, ((x + d) % NX) * NZ + zl)
    for d in range(1, NF):
        greet((f + d) % NF, s)

    loads = [
        pltpu.make_async_copy(src, dst, load_sem.at[n])
        for n, (src, dst) in enumerate(
            [(window_hbm, window), (table_hbm, table), (groups_hbm, groups), (owners_hbm, owners)]
        )
    ]
    chunk = 256
    chunks = 2 * ROWS * SPEC // chunk

    def load_chunk(i):
        rows = pl.ds(pl.multiple_of(i * chunk, chunk), chunk)
        return pltpu.make_async_copy(
            samples_hbm.at[rows, :], samples.at[rows, :], chunk_sem.at[i]
        )

    loads[0].start()
    loads[1].start()
    for i in range(chunks):
        load_chunk(i).start()
    loads[2].start()
    loads[3].start()

    loads[0].wait()
    loads[1].wait()
    taps = table[...] * column(window[...], FFT_LEN)
    high = taps.astype(jnp.bfloat16)
    low = (taps - high.astype(jnp.float32)).astype(jnp.bfloat16)
    both = jnp.concatenate([high, low], axis=0)

    @pl.loop(0, chunks)
    def _(i):
        rows = pl.ds(pl.multiple_of(i * chunk, chunk), chunk)
        load_chunk(i).wait()
        block = samples[rows, :]
        full = jnp.dot(
            jnp.concatenate([block, block], axis=1), both, preferred_element_type=jnp.float32
        )
        uc[rows, :] = full[:, :FFT_LEN]
        us[rows, :] = full[:, FFT_LEN:]

    lane = lax.broadcasted_iota(jnp.int32, (ROWS, 128), 1)
    for t8 in range(SPEC // 8):
        for part in range(2):
            blocks = []
            for t in range(8):
                at = 2 * (t8 * 8 + t)
                re = pl.ds(at, ROWS, stride=2 * SPEC)
                im = pl.ds(at + 1, ROWS, stride=2 * SPEC)
                if part == 0:
                    blocks.append(uc[re, :] + us[im, :])
                else:
                    blocks.append(uc[im, :] - us[re, :])
            blocks = swap_blocks(blocks, AVG, lane)
            for k in range(CH_OUT):
                start = (2 * t8 + part) * 128
                chan[k, :, start : start + 128] = blocks[k].astype(jnp.bfloat16)
    held[s] = chan[zl]
    pl.semaphore_wait(barrier, NZ + NX + NF - 3)

    def block_to(src, at, to_x, to_z):
        return pltpu.make_async_remote_copy(
            src_ref=src,
            dst_ref=held.at[at],
            send_sem=in_send,
            recv_sem=in_recv.at[at],
            device_id=(f, to_x * NZ + to_z),
            device_id_type=MESH,
        )

    def along_x(src, at):
        for dx in (1, 3, 2):
            block_to(src, at, (x + dx) % NX, zl).start()

    steps = (1, 7, 2, 6, 3, 5, 4)
    for dz in steps:
        to = (zl + dz) % NZ
        block_to(chan.at[to], s, x, to).start()
    along_x(chan.at[zl], s)

    loads[2].wait()
    loads[3].wait()
    wide = lax.broadcasted_iota(jnp.int32, (STN, STN), 1)
    tall = lax.broadcasted_iota(jnp.int32, (STN, STN), 0)
    group_row = groups[...]
    row_source = jnp.max(jnp.where(group_row == tall, wide, 0), axis=1, keepdims=True)
    source_row = jnp.max(
        jnp.where(column(group_row, STN) == wide, tall, 0), axis=0, keepdims=True
    )
    place = lax.broadcasted_iota(jnp.int32, (STN, 128), 1)
    sources = jnp.where(place == NZ, row_source, 0)
    for oz in range(NZ):
        picked = jnp.where(owners[...] == x * NZ + oz, source_row, 0)
        sources = jnp.where(place == oz, jnp.max(picked, axis=1, keepdims=True), sources)
    tab_vmem[...] = sources
    to_scalars = pltpu.make_async_copy(tab_vmem, tab, load_sem.at[0])
    to_scalars.start()
    to_scalars.wait()

    for dz in steps:
        at = x * NZ + (zl - dz + NZ) % NZ
        block_to(held.at[at], at, (x + 1) % NX, zl).wait_recv()
        along_x(held.at[at], at)
    for dx in (1, 3, 2):
        for z in range(NZ):
            at = ((x + dx) % NX) * NZ + z
            block_to(held.at[at], at, (x + 1) % NX, zl).wait_recv()

    lane8 = lax.broadcasted_iota(jnp.int32, (8, 128), 1)
    channel = f * CH_OUT + zl

    @pl.loop(0, NF)
    def _(i):
        p = (f + i) % NF
        for r in range(2):
            g1 = 2 * p + r
            a = held[tab[g1, NZ]]
            turned = []
            for t8 in range(SPEC // 8):
                turned.append(a[:, (2 * t8 + 1) * 128 : (2 * t8 + 2) * 128])
                turned.append(-a[:, 2 * t8 * 128 : (2 * t8 + 1) * 128])
            left = jnp.concatenate([a, jnp.concatenate(turned, axis=1)], axis=0)
            right = jnp.concatenate(
                [held[tab[g1, oz]] for oz in range(NZ)], axis=0
            )
            vis = lax.dot_general(
                left, right, (((1,), (1,)), ((), ())), preferred_element_type=jnp.float32
            ) * (1.0 / (AVG * SPEC))
            for h in range(2):
                mixed[r, h] = vis[:, h * 128 : (h + 1) * 128]
                for part in range(2):
                    blocks = [
                        mixed[r, h, pl.ds(part * ROWS + j, 8, stride=4), :] for j in range(4)
                    ]
                    blocks = swap_blocks(blocks, ROWS, lane8)
                    for q in range(4):
                        pairs[4 * h + q, part, pl.ds(r, 8, stride=2), :] = blocks[q]
        outgoing[i] = pairs[...].astype(jnp.bfloat16)
        for oz in range(NZ):
            mine = jnp.logical_and(i == 0, zl == oz)

            @pl.when(jnp.logical_not(mine))
            def _():
                pltpu.make_async_remote_copy(
                    src_ref=outgoing.at[i, oz],
                    dst_ref=out.at[:, channel],
                    send_sem=out_send,
                    recv_sem=out_recv,
                    device_id=(p, x * NZ + oz),
                    device_id_type=MESH,
                ).start()

            @pl.when(mine)
            def _():
                pltpu.make_async_copy(
                    outgoing.at[0, oz], out.at[:, channel], own_sem
                ).start()

    pltpu.make_async_copy(outgoing.at[0, 0], out.at[:, channel], own_sem).wait()
    rest = pltpu.make_async_remote_copy(
        src_ref=out.at[:, pl.ds(0, NF * NZ - 1)],
        dst_ref=out.at[:, pl.ds(0, NF * NZ - 1)],
        send_sem=out_send,
        recv_sem=out_recv,
        device_id=(f, x * NZ + (zl + 1) % NZ),
        device_id_type=MESH,
    )
    rest.wait_send()
    rest.wait_recv()
    sent = pltpu.make_async_remote_copy(
        src_ref=held.at[pl.ds(0, STN - 1)],
        dst_ref=held.at[pl.ds(0, STN - 1)],
        send_sem=in_send,
        recv_sem=in_recv.at[0],
        device_id=(f, x * NZ + (zl + 1) % NZ),
        device_id_type=MESH,
    )
    sent.wait_send()


def shards(samples, window, group_of_device, owner_map):
    flat = samples.reshape(2 * ROWS * SPEC, FFT_LEN)
    hbm = pl.BlockSpec(memory_space=pltpu.HBM)
    got = pl.pallas_call(
        kernel,
        out_shape=jax.ShapeDtypeStruct((2, NF * CH_OUT, 16, 128), jnp.bfloat16),
        in_specs=[hbm] * 5,
        out_specs=pl.BlockSpec(memory_space=pl.ANY),
        scratch_shapes=[
            pltpu.VMEM((2 * ROWS * SPEC, FFT_LEN), jnp.bfloat16),
            pltpu.VMEM((1, FFT_LEN), jnp.float32),
            pltpu.VMEM((1, STN), jnp.int32),
            pltpu.VMEM((STN, STN), jnp.int32),
            pltpu.VMEM((FFT_LEN, 2 * FFT_LEN), jnp.float32),
            pltpu.VMEM((STN, 128), jnp.int32),
            pltpu.SMEM((STN, 128), jnp.int32),
            pltpu.VMEM((2 * ROWS * SPEC, FFT_LEN), jnp.float32),
            pltpu.VMEM((2 * ROWS * SPEC, FFT_LEN), jnp.float32),
            pltpu.VMEM((CH_OUT, ROWS, DEPTH), jnp.bfloat16),
            pltpu.VMEM((STN, ROWS, DEPTH), jnp.bfloat16),
            pltpu.VMEM((2, 2, 2 * ROWS, 128), jnp.float32),
            pltpu.VMEM((NZ, 2, 16, 128), jnp.float32),
            pltpu.VMEM((NF, NZ, 2, 16, 128), jnp.bfloat16),
            pltpu.SemaphoreType.DMA((4,)),
            pltpu.SemaphoreType.DMA((6,)),
            pltpu.SemaphoreType.DMA,
            pltpu.SemaphoreType.DMA((STN,)),
            pltpu.SemaphoreType.DMA,
            pltpu.SemaphoreType.DMA,
            pltpu.SemaphoreType.DMA,
        ],
        compiler_params=pltpu.CompilerParams(
            has_side_effects=True, collective_id=0, vmem_limit_bytes=62 * 1024 * 1024
        ),
        name="correlate_and_regroup",
    )(
        flat,
        window.reshape(1, FFT_LEN),
        group_of_device.reshape(1, STN),
        owner_map,
        jnp.asarray(dft_table()),
    )
    got = got.reshape(2, NF * CH_OUT, 8, 2, 128).transpose(0, 1, 3, 2, 4)
    return got.reshape(2, NF * CH_OUT, 1, 2, ROWS * ROWS)


def solution(mesh):
    return jax.shard_map(
        shards,
        mesh=mesh,
        in_specs=(P("freq", "stn", None, None, None), P(), P(), P()),
        out_specs=P(None, None, "stn", "freq", None),
        check_vma=False,
    )
```

```python
import math

import jax
import jax.numpy as jnp
import numpy as np
from jax import lax
from jax.experimental import pallas as pl
from jax.experimental.pallas import tpu as pltpu
from jax.sharding import PartitionSpec as P

FFT_LEN = 128
AVG = 16
SPEC = 24
CH_OUT = 8
ROWS = 32
DEPTH = 2 * SPEC * AVG
NX = 4
NZ = 8
NF = 16
STN = NX * NZ
MESH = pl.DeviceIdType.MESH
PLAN = ((0, 1), (0, 2), (0, 3), (1, 0), (1, 1), (1, 2), (1, 3))


def dft_table():
    index = np.arange(FFT_LEN)
    theta = (index[:, None] * index[None, :] % FFT_LEN) * (2.0 * math.pi / FFT_LEN)
    table = np.concatenate([np.cos(theta), np.sin(theta)], axis=1) / math.sqrt(FFT_LEN)
    return table.astype(np.float32)


def swap_blocks(blocks, width, lane):
    blocks = list(blocks)
    step = 1
    while step < len(blocks):
        low = (lane // (width * step)) % 2 == 0
        shift = width * step
        for i in range(len(blocks)):
            if i & step:
                continue
            a, b = blocks[i], blocks[i | step]
            blocks[i] = jnp.where(low, a, pltpu.roll(b, shift, 1))
            blocks[i | step] = jnp.where(low, pltpu.roll(a, 128 - shift, 1), b)
        step *= 2
    return blocks


def column(row, size):
    lane = lax.broadcasted_iota(jnp.int32, (size, size), 1)
    sub = lax.broadcasted_iota(jnp.int32, (size, size), 0)
    return jnp.sum(jnp.where(lane == sub, row, jnp.zeros_like(row)), axis=1, keepdims=True)


def kernel(
    samples_hbm, window_hbm, groups_hbm, owners_hbm, table_hbm, out,
    samples, window, groups, owners, table, tab_vmem, tab,
    uc, us, chan, held, mixed, pairs, outgoing,
    load_sem, chunk_sem, in_send, in_recv, out_send, out_recv, own_sem, heard, crossed, known,
):
    f = lax.axis_index("freq")
    s = lax.axis_index("stn")
    x = s // NZ
    zl = s % NZ

    barrier = pltpu.get_barrier_semaphore()
    flip = f + 2 - 4 * ((f // 2) % 2)
    facing = x * NZ + NZ - 1 - zl
    border = jnp.logical_or(zl == 0, zl == NZ - 1)

    def signal(semaphore, to_f, to_s):
        pl.semaphore_signal(semaphore, inc=1, device_id=(to_f, to_s), device_id_type=MESH)

    for d in range(1, NZ):
        signal(barrier, f, x * NZ + (zl + d) % NZ)
    for d in range(1, NX):
        signal(barrier, f, ((x + d) % NX) * NZ + zl)
    for d in range(1, NF // 2):
        y_core = (f // 4 * 2 + f % 2 + d) % (NF // 2)
        signal(barrier, y_core // 2 * 4 + f // 2 % 2 * 2 + y_core % 2, s)

    @pl.when(border)
    def _():
        signal(barrier, flip, facing)

    loads = [
        pltpu.make_async_copy(src, dst, load_sem.at[n])
        for n, (src, dst) in enumerate(
            [(window_hbm, window), (table_hbm, table), (groups_hbm, groups), (owners_hbm, owners)]
        )
    ]
    chunk = 256
    chunks = 2 * ROWS * SPEC // chunk

    def load_chunk(i):
        rows = pl.ds(pl.multiple_of(i * chunk, chunk), chunk)
        return pltpu.make_async_copy(
            samples_hbm.at[rows, :], samples.at[rows, :], chunk_sem.at[i]
        )

    loads[0].start()
    loads[1].start()
    for i in range(chunks):
        load_chunk(i).start()
    loads[2].start()
    loads[3].start()

    loads[0].wait()
    loads[1].wait()
    taps = table[...] * column(window[...], FFT_LEN)
    high = taps.astype(jnp.bfloat16)
    low = (taps - high.astype(jnp.float32)).astype(jnp.bfloat16)
    both = jnp.concatenate([high, low], axis=0)

    @pl.loop(0, chunks)
    def _(i):
        rows = pl.ds(pl.multiple_of(i * chunk, chunk), chunk)
        load_chunk(i).wait()
        block = samples[rows, :]
        full = jnp.dot(
            jnp.concatenate([block, block], axis=1), both, preferred_element_type=jnp.float32
        )
        uc[rows, :] = full[:, :FFT_LEN]
        us[rows, :] = full[:, FFT_LEN:]

    lane = lax.broadcasted_iota(jnp.int32, (ROWS, 128), 1)
    for t8 in range(SPEC // 8):
        for part in range(2):
            blocks = []
            for t in range(8):
                at = 2 * (t8 * 8 + t)
                re = pl.ds(at, ROWS, stride=2 * SPEC)
                im = pl.ds(at + 1, ROWS, stride=2 * SPEC)
                if part == 0:
                    blocks.append(uc[re, :] + us[im, :])
                else:
                    blocks.append(uc[im, :] - us[re, :])
            blocks = swap_blocks(blocks, AVG, lane)
            for k in range(CH_OUT):
                start = (2 * t8 + part) * 128
                chan[k, :, start : start + 128] = blocks[k].astype(jnp.bfloat16)
    held[s] = chan[zl]

    @pl.when(border)
    def _():
        pl.semaphore_wait(barrier, NZ + NX + NF // 2 - 2)

    @pl.when(jnp.logical_not(border))
    def _():
        pl.semaphore_wait(barrier, NZ + NX + NF // 2 - 3)

    @pl.when(zl != NZ - 1)
    def _():
        signal(heard, f, x * NZ + NZ - 1)


    half = NZ // 2

    def turn(n, way):
        other, step = PLAN[n]
        return (zl // half + other) % 2 * half + (zl + half + way * step) % half

    def block_to(src, at, to_x, to_z):
        return pltpu.make_async_remote_copy(
            src_ref=src,
            dst_ref=held.at[at],
            send_sem=in_send,
            recv_sem=in_recv.at[at],
            device_id=(f, to_x * NZ + to_z),
            device_id_type=MESH,
        )

    def share(at):
        for dx in (2, 1, 3):
            block_to(held.at[at], at, (x + dx) % NX, zl).start()

    def arrived(at):
        block_to(held.at[at], at, (x + 1) % NX, zl).wait_recv()

    for n in range(NZ - 1):
        to = turn(n, 1)
        block_to(chan.at[to], s, x, to).start()
    share(s)

    loads[2].wait()
    loads[3].wait()
    wide = lax.broadcasted_iota(jnp.int32, (STN, STN), 1)
    tall = lax.broadcasted_iota(jnp.int32, (STN, STN), 0)
    group_row = groups[...]
    row_source = jnp.max(jnp.where(group_row == tall, wide, 0), axis=1, keepdims=True)
    source_row = jnp.max(
        jnp.where(column(group_row, STN) == wide, tall, 0), axis=0, keepdims=True
    )
    place = lax.broadcasted_iota(jnp.int32, (STN, 128), 1)
    sources = jnp.where(place == NZ, row_source, 0)
    for oz in range(NZ):
        picked = jnp.where(owners[...] == x * NZ + oz, source_row, 0)
        sources = jnp.where(place == oz, jnp.max(picked, axis=1, keepdims=True), sources)
    tab_vmem[...] = sources
    to_scalars = pltpu.make_async_copy(tab_vmem, tab, load_sem.at[0])
    to_scalars.start()
    to_scalars.wait()

    for n in range(NZ - 1):
        at = x * NZ + turn(n, -1)
        arrived(at)
        share(at)
        if n == 3:

            @pl.when(zl == NZ - 1)
            def _():
                pl.semaphore_wait(heard, NZ - 1)
                signal(crossed, flip, facing)

        if n == 5:

            @pl.when(zl == 0)
            def _():
                pl.semaphore_wait(crossed, 1)
                for z in range(1, NZ):
                    signal(known, f, x * NZ + z)

    for dx in range(1, NX):
        for z in range(NZ):
            arrived((x + dx) % NX * NZ + z)

    @pl.when(zl != 0)
    def _():
        pl.semaphore_wait(known, 1)

    lane8 = lax.broadcasted_iota(jnp.int32, (8, 128), 1)
    channel = f * CH_OUT + zl

    @pl.loop(0, NF)
    def _(i):
        p = (f + i) % NF
        for r in range(2):
            g1 = 2 * p + r
            a = held[tab[g1, NZ]]
            turned = []
            for t8 in range(SPEC // 8):
                turned.append(a[:, (2 * t8 + 1) * 128 : (2 * t8 + 2) * 128])
                turned.append(-a[:, 2 * t8 * 128 : (2 * t8 + 1) * 128])
            left = jnp.concatenate([a, jnp.concatenate(turned, axis=1)], axis=0)
            right = jnp.concatenate(
                [held[tab[g1, oz]] for oz in range(NZ)], axis=0
            )
            vis = lax.dot_general(
                left, right, (((1,), (1,)), ((), ())), preferred_element_type=jnp.float32
            ) * (1.0 / (AVG * SPEC))
            for h in range(2):
                mixed[r, h] = vis[:, h * 128 : (h + 1) * 128]
                for part in range(2):
                    blocks = [
                        mixed[r, h, pl.ds(part * ROWS + j, 8, stride=4), :] for j in range(4)
                    ]
                    blocks = swap_blocks(blocks, ROWS, lane8)
                    for q in range(4):
                        pairs[4 * h + q, part, pl.ds(r, 8, stride=2), :] = blocks[q]
        outgoing[i] = pairs[...].astype(jnp.bfloat16)
        for oz in range(NZ):
            mine = jnp.logical_and(i == 0, zl == oz)

            @pl.when(jnp.logical_not(mine))
            def _():
                pltpu.make_async_remote_copy(
                    src_ref=outgoing.at[i, oz],
                    dst_ref=out.at[:, channel],
                    send_sem=out_send,
                    recv_sem=out_recv,
                    device_id=(p, x * NZ + oz),
                    device_id_type=MESH,
                ).start()

            @pl.when(mine)
            def _():
                pltpu.make_async_copy(
                    outgoing.at[0, oz], out.at[:, channel], own_sem
                ).start()

    pltpu.make_async_copy(outgoing.at[0, 0], out.at[:, channel], own_sem).wait()
    rest = pltpu.make_async_remote_copy(
        src_ref=out.at[:, pl.ds(0, NF * NZ - 1)],
        dst_ref=out.at[:, pl.ds(0, NF * NZ - 1)],
        send_sem=out_send,
        recv_sem=out_recv,
        device_id=(f, x * NZ + (zl + 1) % NZ),
        device_id_type=MESH,
    )
    rest.wait_send()
    rest.wait_recv()
    sent = pltpu.make_async_remote_copy(
        src_ref=held.at[pl.ds(0, STN - 1)],
        dst_ref=held.at[pl.ds(0, STN - 1)],
        send_sem=in_send,
        recv_sem=in_recv.at[0],
        device_id=(f, x * NZ + (zl + 1) % NZ),
        device_id_type=MESH,
    )
    sent.wait_send()


def shards(samples, window, group_of_device, owner_map):
    flat = samples.reshape(2 * ROWS * SPEC, FFT_LEN)
    hbm = pl.BlockSpec(memory_space=pltpu.HBM)
    got = pl.pallas_call(
        kernel,
        out_shape=jax.ShapeDtypeStruct((2, NF * CH_OUT, 16, 128), jnp.bfloat16),
        in_specs=[hbm] * 5,
        out_specs=pl.BlockSpec(memory_space=pl.ANY),
        scratch_shapes=[
            pltpu.VMEM((2 * ROWS * SPEC, FFT_LEN), jnp.bfloat16),
            pltpu.VMEM((1, FFT_LEN), jnp.float32),
            pltpu.VMEM((1, STN), jnp.int32),
            pltpu.VMEM((STN, STN), jnp.int32),
            pltpu.VMEM((FFT_LEN, 2 * FFT_LEN), jnp.float32),
            pltpu.VMEM((STN, 128), jnp.int32),
            pltpu.SMEM((STN, 128), jnp.int32),
            pltpu.VMEM((2 * ROWS * SPEC, FFT_LEN), jnp.float32),
            pltpu.VMEM((2 * ROWS * SPEC, FFT_LEN), jnp.float32),
            pltpu.VMEM((CH_OUT, ROWS, DEPTH), jnp.bfloat16),
            pltpu.VMEM((STN, ROWS, DEPTH), jnp.bfloat16),
            pltpu.VMEM((2, 2, 2 * ROWS, 128), jnp.float32),
            pltpu.VMEM((NZ, 2, 16, 128), jnp.float32),
            pltpu.VMEM((NF, NZ, 2, 16, 128), jnp.bfloat16),
            pltpu.SemaphoreType.DMA((4,)),
            pltpu.SemaphoreType.DMA((6,)),
            pltpu.SemaphoreType.DMA,
            pltpu.SemaphoreType.DMA((STN,)),
            pltpu.SemaphoreType.DMA,
            pltpu.SemaphoreType.DMA,
            pltpu.SemaphoreType.DMA,
            pltpu.SemaphoreType.REGULAR,
            pltpu.SemaphoreType.REGULAR,
            pltpu.SemaphoreType.REGULAR,
        ],
        compiler_params=pltpu.CompilerParams(
            has_side_effects=True, collective_id=0, vmem_limit_bytes=32 * 1024 * 1024
        ),
        name="correlate_and_regroup",
    )(
        *(
            pltpu.with_memory_space_constraint(operand, pltpu.HBM)
            for operand in (
                flat,
                window.reshape(1, FFT_LEN),
                group_of_device.reshape(1, STN),
                owner_map,
                jnp.asarray(dft_table()),
            )
        )
    )
    got = got.reshape(2, NF * CH_OUT, 8, 2, 128).transpose(0, 1, 3, 2, 4)
    return got.reshape(2, NF * CH_OUT, 1, 2, ROWS * ROWS)


def solution(mesh):
    return jax.shard_map(
        shards,
        mesh=mesh,
        in_specs=(P("freq", "stn", None, None, None), P(), P(), P()),
        out_specs=P(None, None, "stn", "freq", None),
        check_vma=False,
    )
```

```python
import math

import jax
import jax.numpy as jnp
import numpy as np
from jax import lax
from jax.experimental import pallas as pl
from jax.experimental.pallas import tpu as pltpu
from jax.sharding import PartitionSpec as P

FFT_LEN = 128
AVG = 16
SPEC = 24
CH_OUT = 8
ROWS = 32
DEPTH = 2 * SPEC * AVG
NX = 4
NZ = 8
NF = 16
STN = NX * NZ
MESH = pl.DeviceIdType.MESH
PLAN = ((0, 1), (0, 2), (0, 3), (1, 0), (1, 1), (1, 2), (1, 3))
RELAYED = 0


def dft_table():
    index = np.arange(FFT_LEN)
    theta = (index[:, None] * index[None, :] % FFT_LEN) * (2.0 * math.pi / FFT_LEN)
    table = np.concatenate([np.cos(theta), np.sin(theta)], axis=1) / math.sqrt(FFT_LEN)
    return table.astype(np.float32)


def swap_blocks(blocks, width, lane):
    blocks = list(blocks)
    step = 1
    while step < len(blocks):
        low = (lane // (width * step)) % 2 == 0
        shift = width * step
        for i in range(len(blocks)):
            if i & step:
                continue
            a, b = blocks[i], blocks[i | step]
            blocks[i] = jnp.where(low, a, pltpu.roll(b, shift, 1))
            blocks[i | step] = jnp.where(low, pltpu.roll(a, 128 - shift, 1), b)
        step *= 2
    return blocks


def column(row, size):
    lane = lax.broadcasted_iota(jnp.int32, (size, size), 1)
    sub = lax.broadcasted_iota(jnp.int32, (size, size), 0)
    return jnp.sum(jnp.where(lane == sub, row, jnp.zeros_like(row)), axis=1, keepdims=True)


def kernel(
    samples_hbm, window_hbm, groups_hbm, owners_hbm, table_hbm, out,
    samples, window, groups, owners, table, tab_vmem, tab,
    uc, us, chan, held, mixed, pairs, outgoing,
    load_sem, chunk_sem, in_send, in_recv, out_send, out_recv, own_sem, heard, crossed, known, go,
):
    f = lax.axis_index("freq")
    s = lax.axis_index("stn")
    x = s // NZ
    zl = s % NZ

    barrier = pltpu.get_barrier_semaphore()
    flip = f + 2 - 4 * ((f // 2) % 2)
    facing = x * NZ + NZ - 1 - zl
    border = jnp.logical_or(zl == 0, zl == NZ - 1)

    def signal(semaphore, to_f, to_s):
        pl.semaphore_signal(semaphore, inc=1, device_id=(to_f, to_s), device_id_type=MESH)

    for d in range(1, NZ):
        signal(barrier, f, x * NZ + (zl + d) % NZ)
    for d in range(1, NX):
        signal(barrier, f, ((x + d) % NX) * NZ + zl)
    for d in range(1, NF // 2):
        y_core = (f // 4 * 2 + f % 2 + d) % (NF // 2)
        signal(barrier, y_core // 2 * 4 + f // 2 % 2 * 2 + y_core % 2, s)

    @pl.when(border)
    def _():
        signal(barrier, flip, facing)

    loads = [
        pltpu.make_async_copy(src, dst, load_sem.at[n])
        for n, (src, dst) in enumerate(
            [(window_hbm, window), (table_hbm, table), (groups_hbm, groups), (owners_hbm, owners)]
        )
    ]
    chunk = 256
    chunks = 2 * ROWS * SPEC // chunk

    def load_chunk(i):
        rows = pl.ds(pl.multiple_of(i * chunk, chunk), chunk)
        return pltpu.make_async_copy(
            samples_hbm.at[rows, :], samples.at[rows, :], chunk_sem.at[i]
        )

    loads[0].start()
    loads[1].start()
    for i in range(chunks):
        load_chunk(i).start()
    loads[2].start()
    loads[3].start()

    loads[0].wait()
    loads[1].wait()
    taps = table[...] * column(window[...], FFT_LEN)
    high = taps.astype(jnp.bfloat16)
    low = (taps - high.astype(jnp.float32)).astype(jnp.bfloat16)
    both = jnp.concatenate([high, low], axis=0)

    @pl.loop(0, chunks)
    def _(i):
        rows = pl.ds(pl.multiple_of(i * chunk, chunk), chunk)
        load_chunk(i).wait()
        block = samples[rows, :]
        full = jnp.dot(
            jnp.concatenate([block, block], axis=1), both, preferred_element_type=jnp.float32
        )
        uc[rows, :] = full[:, :FFT_LEN]
        us[rows, :] = full[:, FFT_LEN:]

    lane = lax.broadcasted_iota(jnp.int32, (ROWS, 128), 1)
    for t8 in range(SPEC // 8):
        for part in range(2):
            blocks = []
            for t in range(8):
                at = 2 * (t8 * 8 + t)
                re = pl.ds(at, ROWS, stride=2 * SPEC)
                im = pl.ds(at + 1, ROWS, stride=2 * SPEC)
                if part == 0:
                    blocks.append(uc[re, :] + us[im, :])
                else:
                    blocks.append(uc[im, :] - us[re, :])
            blocks = swap_blocks(blocks, AVG, lane)
            for k in range(CH_OUT):
                start = (2 * t8 + part) * 128
                chan[k, :, start : start + 128] = blocks[k].astype(jnp.bfloat16)
    held[s] = chan[zl]

    @pl.when(border)
    def _():
        pl.semaphore_wait(barrier, NZ + NX + NF // 2 - 2)

    @pl.when(jnp.logical_not(border))
    def _():
        pl.semaphore_wait(barrier, NZ + NX + NF // 2 - 3)

    @pl.when(zl != NZ - 1)
    def _():
        signal(heard, f, x * NZ + NZ - 1)


    half = NZ // 2

    def turn(n):
        other, step = PLAN[n]
        high = (zl // 2 + step // 2) % 2
        low = (zl + step) % 2
        return (zl // half + other) % 2 * half + high * 2 + low

    def block_to(src, at, to_x, to_z):
        return pltpu.make_async_remote_copy(
            src_ref=src,
            dst_ref=held.at[at],
            send_sem=in_send,
            recv_sem=in_recv.at[at],
            device_id=(f, to_x * NZ + to_z),
            device_id_type=MESH,
        )

    right = (x + 1) % NX
    left = (x + 3) % NX

    def forward(at, to_x):
        block_to(held.at[at], at, to_x, zl).start()

    def place_of(of_x, n):
        return of_x * NZ + (turn(n) if n >= 0 else zl)

    def share(n):
        at = place_of(x, n)
        if n + 1 >= RELAYED:
            forward(at, (x + 2) % NX)
        forward(at, right if n % 2 else left)
        forward(at, left if n % 2 else right)

    def arrived(at):
        block_to(held.at[at], at, right, zl).wait_recv()

    def relay(n):
        came, to_x = (left, right) if n % 2 else (right, left)
        at = place_of(came, n)
        arrived(at)
        forward(at, to_x)

    core = f % 2

    @pl.when(core == 0)
    def _():
        for n in range(NZ - 1):
            to = turn(n)
            block_to(chan.at[to], s, x, to).start()

    share(-1)

    loads[2].wait()
    loads[3].wait()
    wide = lax.broadcasted_iota(jnp.int32, (STN, STN), 1)
    tall = lax.broadcasted_iota(jnp.int32, (STN, STN), 0)
    group_row = groups[...]
    row_source = jnp.max(jnp.where(group_row == tall, wide, 0), axis=1, keepdims=True)
    source_row = jnp.max(
        jnp.where(column(group_row, STN) == wide, tall, 0), axis=0, keepdims=True
    )
    place = lax.broadcasted_iota(jnp.int32, (STN, 128), 1)
    sources = jnp.where(place == NZ, row_source, 0)
    for oz in range(NZ):
        picked = jnp.where(owners[...] == x * NZ + oz, source_row, 0)
        sources = jnp.where(place == oz, jnp.max(picked, axis=1, keepdims=True), sources)
    tab_vmem[...] = sources
    to_scalars = pltpu.make_async_copy(tab_vmem, tab, load_sem.at[0])
    to_scalars.start()
    to_scalars.wait()

    @pl.when(core == 1)
    def _():
        pl.semaphore_wait(go, 1)
        for n in range(NZ - 1):
            to = turn(n)
            block_to(chan.at[to], s, x, to).start()

    for n in range(NZ - 1):
        arrived(place_of(x, n))
        share(n)
        if n - 2 >= -1 and n - 1 < RELAYED:
            relay(n - 2)
        if n == 6:

            @pl.when(core == 0)
            def _():
                signal(go, f + 1, s)

        if n == 3:

            @pl.when(zl == NZ - 1)
            def _():
                pl.semaphore_wait(heard, NZ - 1)
                signal(crossed, flip, facing)

        if n == 5:

            @pl.when(zl == 0)
            def _():
                pl.semaphore_wait(crossed, 1)
                for z in range(1, NZ):
                    signal(known, f, x * NZ + z)

    for n in range(-1, NZ - 1):
        if n + 1 < RELAYED:
            arrived(place_of(right if n % 2 else left, n))
        else:
            arrived(place_of(left, n))
            arrived(place_of(right, n))
        arrived(place_of((x + 2) % NX, n))

    @pl.when(zl != 0)
    def _():
        pl.semaphore_wait(known, 1)

    lane8 = lax.broadcasted_iota(jnp.int32, (8, 128), 1)
    channel = f * CH_OUT + zl

    @pl.loop(0, NF)
    def _(i):
        y_core = (f // 4 * 2 + f % 2 + i) % (NF // 2)
        p = y_core // 2 * 4 + (f // 2 + 1 + i // (NF // 2)) % 2 * 2 + y_core % 2
        for r in range(2):
            g1 = 2 * p + r
            a = held[tab[g1, NZ]]
            turned = []
            for t8 in range(SPEC // 8):
                turned.append(a[:, (2 * t8 + 1) * 128 : (2 * t8 + 2) * 128])
                turned.append(-a[:, 2 * t8 * 128 : (2 * t8 + 1) * 128])
            left = jnp.concatenate([a, jnp.concatenate(turned, axis=1)], axis=0)
            right = jnp.concatenate(
                [held[tab[g1, oz]] for oz in range(NZ)], axis=0
            )
            vis = lax.dot_general(
                left, right, (((1,), (1,)), ((), ())), preferred_element_type=jnp.float32
            ) * (1.0 / (AVG * SPEC))
            for h in range(2):
                mixed[r, h] = vis[:, h * 128 : (h + 1) * 128]
                for part in range(2):
                    blocks = [
                        mixed[r, h, pl.ds(part * ROWS + j, 8, stride=4), :] for j in range(4)
                    ]
                    blocks = swap_blocks(blocks, ROWS, lane8)
                    for q in range(4):
                        pairs[4 * h + q, part, pl.ds(r, 8, stride=2), :] = blocks[q]
        outgoing[i] = pairs[...].astype(jnp.bfloat16)
        for d in range(NZ):
            oz = (zl + d) % NZ
            mine = jnp.logical_and(p == f, d == 0)

            @pl.when(jnp.logical_not(mine))
            def _():
                pltpu.make_async_remote_copy(
                    src_ref=outgoing.at[i, oz],
                    dst_ref=out.at[:, channel],
                    send_sem=out_send,
                    recv_sem=out_recv,
                    device_id=(p, x * NZ + oz),
                    device_id_type=MESH,
                ).start()

            @pl.when(mine)
            def _():
                pltpu.make_async_copy(
                    outgoing.at[i, oz], out.at[:, channel], own_sem
                ).start()

    pltpu.make_async_copy(outgoing.at[0, 0], out.at[:, channel], own_sem).wait()
    rest = pltpu.make_async_remote_copy(
        src_ref=out.at[:, pl.ds(0, NF * NZ - 1)],
        dst_ref=out.at[:, pl.ds(0, NF * NZ - 1)],
        send_sem=out_send,
        recv_sem=out_recv,
        device_id=(f, x * NZ + (zl + 1) % NZ),
        device_id_type=MESH,
    )
    rest.wait_send()
    rest.wait_recv()
    sent = pltpu.make_async_remote_copy(
        src_ref=held.at[pl.ds(0, STN - 1)],
        dst_ref=held.at[pl.ds(0, STN - 1)],
        send_sem=in_send,
        recv_sem=in_recv.at[0],
        device_id=(f, x * NZ + (zl + 1) % NZ),
        device_id_type=MESH,
    )
    sent.wait_send()


def shards(samples, window, group_of_device, owner_map):
    flat = samples.reshape(2 * ROWS * SPEC, FFT_LEN)
    hbm = pl.BlockSpec(memory_space=pltpu.HBM)
    got = pl.pallas_call(
        kernel,
        out_shape=jax.ShapeDtypeStruct((2, NF * CH_OUT, 16, 128), jnp.bfloat16),
        in_specs=[hbm] * 5,
        out_specs=pl.BlockSpec(memory_space=pl.ANY),
        scratch_shapes=[
            pltpu.VMEM((2 * ROWS * SPEC, FFT_LEN), jnp.bfloat16),
            pltpu.VMEM((1, FFT_LEN), jnp.float32),
            pltpu.VMEM((1, STN), jnp.int32),
            pltpu.VMEM((STN, STN), jnp.int32),
            pltpu.VMEM((FFT_LEN, 2 * FFT_LEN), jnp.float32),
            pltpu.VMEM((STN, 128), jnp.int32),
            pltpu.SMEM((STN, 128), jnp.int32),
            pltpu.VMEM((2 * ROWS * SPEC, FFT_LEN), jnp.float32),
            pltpu.VMEM((2 * ROWS * SPEC, FFT_LEN), jnp.float32),
            pltpu.VMEM((CH_OUT, ROWS, DEPTH), jnp.bfloat16),
            pltpu.VMEM((STN, ROWS, DEPTH), jnp.bfloat16),
            pltpu.VMEM((2, 2, 2 * ROWS, 128), jnp.float32),
            pltpu.VMEM((NZ, 2, 16, 128), jnp.float32),
            pltpu.VMEM((NF, NZ, 2, 16, 128), jnp.bfloat16),
            pltpu.SemaphoreType.DMA((4,)),
            pltpu.SemaphoreType.DMA((6,)),
            pltpu.SemaphoreType.DMA,
            pltpu.SemaphoreType.DMA((STN,)),
            pltpu.SemaphoreType.DMA,
            pltpu.SemaphoreType.DMA,
            pltpu.SemaphoreType.DMA,
            pltpu.SemaphoreType.REGULAR,
            pltpu.SemaphoreType.REGULAR,
            pltpu.SemaphoreType.REGULAR,
            pltpu.SemaphoreType.REGULAR,
        ],
        compiler_params=pltpu.CompilerParams(
            has_side_effects=True, collective_id=0, vmem_limit_bytes=32 * 1024 * 1024
        ),
        name="correlate_and_regroup",
    )(
        *(
            pltpu.with_memory_space_constraint(operand, pltpu.HBM)
            for operand in (
                flat,
                window.reshape(1, FFT_LEN),
                group_of_device.reshape(1, STN),
                owner_map,
                jnp.asarray(dft_table()),
            )
        )
    )
    got = got.reshape(2, NF * CH_OUT, 8, 2, 128).transpose(0, 1, 3, 2, 4)
    return got.reshape(2, NF * CH_OUT, 1, 2, ROWS * ROWS)


def solution(mesh):
    return jax.shard_map(
        shards,
        mesh=mesh,
        in_specs=(P("freq", "stn", None, None, None), P(), P(), P()),
        out_specs=P(None, None, "stn", "freq", None),
        check_vma=False,
    )
```

```python
import math

import jax
import jax.numpy as jnp
import numpy as np
from jax import lax
from jax.experimental import pallas as pl
from jax.experimental.pallas import tpu as pltpu
from jax.sharding import PartitionSpec as P

FFT_LEN = 128
AVG = 16
SPEC = 24
CH_OUT = 8
ROWS = 32
DEPTH = 2 * SPEC * AVG
NX = 4
NZ = 8
NF = 16
STN = NX * NZ
MESH = pl.DeviceIdType.MESH
PLAN = ((0, 1), (0, 2), (0, 3), (1, 0), (1, 1), (1, 2), (1, 3))
RELAYED = 0


def dft_table():
    index = np.arange(FFT_LEN)
    theta = (index[:, None] * index[None, :] % FFT_LEN) * (2.0 * math.pi / FFT_LEN)
    table = np.concatenate([np.cos(theta), np.sin(theta)], axis=1) / math.sqrt(FFT_LEN)
    return table.astype(np.float32)


def swap_blocks(blocks, width, lane):
    blocks = list(blocks)
    step = 1
    while step < len(blocks):
        low = (lane // (width * step)) % 2 == 0
        shift = width * step
        for i in range(len(blocks)):
            if i & step:
                continue
            a, b = blocks[i], blocks[i | step]
            blocks[i] = jnp.where(low, a, pltpu.roll(b, shift, 1))
            blocks[i | step] = jnp.where(low, pltpu.roll(a, 128 - shift, 1), b)
        step *= 2
    return blocks


def column(row, size):
    lane = lax.broadcasted_iota(jnp.int32, (size, size), 1)
    sub = lax.broadcasted_iota(jnp.int32, (size, size), 0)
    return jnp.sum(jnp.where(lane == sub, row, jnp.zeros_like(row)), axis=1, keepdims=True)


def kernel(
    samples_hbm, window_hbm, groups_hbm, owners_hbm, table_hbm, out,
    samples, window, groups, owners, table, tab_vmem, tab,
    uc, us, chan, held, mixed, pairs, outgoing,
    load_sem, chunk_sem, in_send, in_recv, out_send, out_recv, own_sem, heard, crossed, known, go,
):
    f = lax.axis_index("freq")
    s = lax.axis_index("stn")
    x = s // NZ
    zl = s % NZ

    barrier = pltpu.get_barrier_semaphore()
    flip = f + 2 - 4 * ((f // 2) % 2)
    facing = x * NZ + NZ - 1 - zl
    border = jnp.logical_or(zl == 0, zl == NZ - 1)

    def signal(semaphore, to_f, to_s):
        pl.semaphore_signal(semaphore, inc=1, device_id=(to_f, to_s), device_id_type=MESH)

    for d in range(1, NZ):
        signal(barrier, f, x * NZ + (zl + d) % NZ)
    for d in range(1, NX):
        signal(barrier, f, ((x + d) % NX) * NZ + zl)
    for d in range(1, NF // 2):
        y_core = (f // 4 * 2 + f % 2 + d) % (NF // 2)
        signal(barrier, y_core // 2 * 4 + f // 2 % 2 * 2 + y_core % 2, s)

    @pl.when(border)
    def _():
        signal(barrier, flip, facing)

    loads = [
        pltpu.make_async_copy(src, dst, load_sem.at[n])
        for n, (src, dst) in enumerate(
            [(window_hbm, window), (table_hbm, table), (groups_hbm, groups), (owners_hbm, owners)]
        )
    ]
    chunk = 256
    chunks = 2 * ROWS * SPEC // chunk

    def load_chunk(i):
        rows = pl.ds(pl.multiple_of(i * chunk, chunk), chunk)
        return pltpu.make_async_copy(
            samples_hbm.at[rows, :], samples.at[rows, :], chunk_sem.at[i]
        )

    loads[0].start()
    loads[1].start()
    for i in range(chunks):
        load_chunk(i).start()
    loads[2].start()
    loads[3].start()

    loads[0].wait()
    loads[1].wait()
    taps = table[...] * column(window[...], FFT_LEN)
    high = taps.astype(jnp.bfloat16)
    low = (taps - high.astype(jnp.float32)).astype(jnp.bfloat16)
    both = jnp.concatenate([high, low], axis=0)

    @pl.loop(0, chunks)
    def _(i):
        rows = pl.ds(pl.multiple_of(i * chunk, chunk), chunk)
        load_chunk(i).wait()
        block = samples[rows, :]
        full = jnp.dot(
            jnp.concatenate([block, block], axis=1), both, preferred_element_type=jnp.float32
        )
        uc[rows, :] = full[:, :FFT_LEN]
        us[rows, :] = full[:, FFT_LEN:]

    lane = lax.broadcasted_iota(jnp.int32, (ROWS, 128), 1)
    for t8 in range(SPEC // 8):
        for part in range(2):
            blocks = []
            for t in range(8):
                at = 2 * (t8 * 8 + t)
                re = pl.ds(at, ROWS, stride=2 * SPEC)
                im = pl.ds(at + 1, ROWS, stride=2 * SPEC)
                if part == 0:
                    blocks.append(uc[re, :] + us[im, :])
                else:
                    blocks.append(uc[im, :] - us[re, :])
            blocks = swap_blocks(blocks, AVG, lane)
            for k in range(CH_OUT):
                start = (2 * t8 + part) * 128
                chan[k, :, start : start + 128] = blocks[k].astype(jnp.bfloat16)
    held[s] = chan[zl]

    @pl.when(border)
    def _():
        pl.semaphore_wait(barrier, NZ + NX + NF // 2 - 2)

    @pl.when(jnp.logical_not(border))
    def _():
        pl.semaphore_wait(barrier, NZ + NX + NF // 2 - 3)

    @pl.when(zl != NZ - 1)
    def _():
        signal(heard, f, x * NZ + NZ - 1)


    half = NZ // 2

    def turn(n):
        other, step = PLAN[n]
        high = (zl // 2 + step // 2) % 2
        low = (zl + step) % 2
        return (zl // half + other) % 2 * half + high * 2 + low

    def block_to(src, at, to_x, to_z):
        return pltpu.make_async_remote_copy(
            src_ref=src,
            dst_ref=held.at[at],
            send_sem=in_send,
            recv_sem=in_recv.at[at],
            device_id=(f, to_x * NZ + to_z),
            device_id_type=MESH,
        )

    right = (x + 1) % NX
    left = (x + 3) % NX

    def forward(at, to_x):
        block_to(held.at[at], at, to_x, zl).start()

    def place_of(of_x, n):
        return of_x * NZ + (turn(n) if n >= 0 else zl)

    def share(n):
        at = place_of(x, n)
        if n + 1 >= RELAYED:
            forward(at, (x + 2) % NX)
        forward(at, right if n % 2 else left)
        forward(at, left if n % 2 else right)

    def arrived(at):
        block_to(held.at[at], at, right, zl).wait_recv()

    def relay(n):
        came, to_x = (left, right) if n % 2 else (right, left)
        at = place_of(came, n)
        arrived(at)
        forward(at, to_x)

    second = 1 - f % 2

    @pl.when(second == 0)
    def _():
        for n in range(NZ - 1):
            to = turn(n)
            block_to(chan.at[to], s, x, to).start()

    share(-1)

    loads[2].wait()
    loads[3].wait()
    wide = lax.broadcasted_iota(jnp.int32, (STN, STN), 1)
    tall = lax.broadcasted_iota(jnp.int32, (STN, STN), 0)
    group_row = groups[...]
    row_source = jnp.max(jnp.where(group_row == tall, wide, 0), axis=1, keepdims=True)
    source_row = jnp.max(
        jnp.where(column(group_row, STN) == wide, tall, 0), axis=0, keepdims=True
    )
    place = lax.broadcasted_iota(jnp.int32, (STN, 128), 1)
    sources = jnp.where(place == NZ, row_source, 0)
    for oz in range(NZ):
        picked = jnp.where(owners[...] == x * NZ + oz, source_row, 0)
        sources = jnp.where(place == oz, jnp.max(picked, axis=1, keepdims=True), sources)
    tab_vmem[...] = sources
    to_scalars = pltpu.make_async_copy(tab_vmem, tab, load_sem.at[0])
    to_scalars.start()
    to_scalars.wait()

    @pl.when(second == 1)
    def _():
        pl.semaphore_wait(go, 1)
        for n in range(NZ - 1):
            to = turn(n)
            block_to(chan.at[to], s, x, to).start()

    for n in range(NZ - 1):
        arrived(place_of(x, n))
        share(n)
        if n - 2 >= -1 and n - 1 < RELAYED:
            relay(n - 2)
        if n == 5:

            @pl.when(second == 0)
            def _():
                signal(go, f - 1, s)

        if n == 3:

            @pl.when(zl == NZ - 1)
            def _():
                pl.semaphore_wait(heard, NZ - 1)
                signal(crossed, flip, facing)

        if n == 5:

            @pl.when(zl == 0)
            def _():
                pl.semaphore_wait(crossed, 1)
                for z in range(1, NZ):
                    signal(known, f, x * NZ + z)

    for n in range(-1, NZ - 1):
        if n + 1 < RELAYED:
            arrived(place_of(right if n % 2 else left, n))
        else:
            arrived(place_of(left, n))
            arrived(place_of(right, n))
        arrived(place_of((x + 2) % NX, n))

    @pl.when(zl != 0)
    def _():
        pl.semaphore_wait(known, 1)

    lane8 = lax.broadcasted_iota(jnp.int32, (8, 128), 1)
    channel = f * CH_OUT + zl

    @pl.loop(0, NF)
    def _(i):
        y_core = (f // 4 * 2 + f % 2 + i) % (NF // 2)
        p = y_core // 2 * 4 + (f // 2 + 1 + i // (NF // 2)) % 2 * 2 + y_core % 2
        for r in range(2):
            g1 = 2 * p + r
            a = held[tab[g1, NZ]]
            turned = []
            for t8 in range(SPEC // 8):
                turned.append(a[:, (2 * t8 + 1) * 128 : (2 * t8 + 2) * 128])
                turned.append(-a[:, 2 * t8 * 128 : (2 * t8 + 1) * 128])
            left = jnp.concatenate([a, jnp.concatenate(turned, axis=1)], axis=0)
            right = jnp.concatenate(
                [held[tab[g1, oz]] for oz in range(NZ)], axis=0
            )
            vis = lax.dot_general(
                left, right, (((1,), (1,)), ((), ())), preferred_element_type=jnp.float32
            ) * (1.0 / (AVG * SPEC))
            for h in range(2):
                mixed[r, h] = vis[:, h * 128 : (h + 1) * 128]
                for part in range(2):
                    blocks = [
                        mixed[r, h, pl.ds(part * ROWS + j, 8, stride=4), :] for j in range(4)
                    ]
                    blocks = swap_blocks(blocks, ROWS, lane8)
                    for q in range(4):
                        pairs[4 * h + q, part, pl.ds(r, 8, stride=2), :] = blocks[q]
        outgoing[i] = pairs[...].astype(jnp.bfloat16)
        for d in range(NZ):
            oz = (zl + d) % NZ
            mine = jnp.logical_and(p == f, d == 0)

            @pl.when(jnp.logical_not(mine))
            def _():
                pltpu.make_async_remote_copy(
                    src_ref=outgoing.at[i, oz],
                    dst_ref=out.at[:, channel],
                    send_sem=out_send,
                    recv_sem=out_recv,
                    device_id=(p, x * NZ + oz),
                    device_id_type=MESH,
                ).start()

            @pl.when(mine)
            def _():
                pltpu.make_async_copy(
                    outgoing.at[i, oz], out.at[:, channel], own_sem
                ).start()

    pltpu.make_async_copy(outgoing.at[0, 0], out.at[:, channel], own_sem).wait()
    rest = pltpu.make_async_remote_copy(
        src_ref=out.at[:, pl.ds(0, NF * NZ - 1)],
        dst_ref=out.at[:, pl.ds(0, NF * NZ - 1)],
        send_sem=out_send,
        recv_sem=out_recv,
        device_id=(f, x * NZ + (zl + 1) % NZ),
        device_id_type=MESH,
    )
    rest.wait_send()
    rest.wait_recv()
    sent = pltpu.make_async_remote_copy(
        src_ref=held.at[pl.ds(0, STN - 1)],
        dst_ref=held.at[pl.ds(0, STN - 1)],
        send_sem=in_send,
        recv_sem=in_recv.at[0],
        device_id=(f, x * NZ + (zl + 1) % NZ),
        device_id_type=MESH,
    )
    sent.wait_send()


def shards(samples, window, group_of_device, owner_map):
    flat = samples.reshape(2 * ROWS * SPEC, FFT_LEN)
    hbm = pl.BlockSpec(memory_space=pltpu.HBM)
    got = pl.pallas_call(
        kernel,
        out_shape=jax.ShapeDtypeStruct((2, NF * CH_OUT, 16, 128), jnp.bfloat16),
        in_specs=[hbm] * 5,
        out_specs=pl.BlockSpec(memory_space=pl.ANY),
        scratch_shapes=[
            pltpu.VMEM((2 * ROWS * SPEC, FFT_LEN), jnp.bfloat16),
            pltpu.VMEM((1, FFT_LEN), jnp.float32),
            pltpu.VMEM((1, STN), jnp.int32),
            pltpu.VMEM((STN, STN), jnp.int32),
            pltpu.VMEM((FFT_LEN, 2 * FFT_LEN), jnp.float32),
            pltpu.VMEM((STN, 128), jnp.int32),
            pltpu.SMEM((STN, 128), jnp.int32),
            pltpu.VMEM((2 * ROWS * SPEC, FFT_LEN), jnp.float32),
            pltpu.VMEM((2 * ROWS * SPEC, FFT_LEN), jnp.float32),
            pltpu.VMEM((CH_OUT, ROWS, DEPTH), jnp.bfloat16),
            pltpu.VMEM((STN, ROWS, DEPTH), jnp.bfloat16),
            pltpu.VMEM((2, 2, 2 * ROWS, 128), jnp.float32),
            pltpu.VMEM((NZ, 2, 16, 128), jnp.float32),
            pltpu.VMEM((NF, NZ, 2, 16, 128), jnp.bfloat16),
            pltpu.SemaphoreType.DMA((4,)),
            pltpu.SemaphoreType.DMA((6,)),
            pltpu.SemaphoreType.DMA,
            pltpu.SemaphoreType.DMA((STN,)),
            pltpu.SemaphoreType.DMA,
            pltpu.SemaphoreType.DMA,
            pltpu.SemaphoreType.DMA,
            pltpu.SemaphoreType.REGULAR,
            pltpu.SemaphoreType.REGULAR,
            pltpu.SemaphoreType.REGULAR,
            pltpu.SemaphoreType.REGULAR,
        ],
        compiler_params=pltpu.CompilerParams(
            has_side_effects=True, collective_id=0, vmem_limit_bytes=32 * 1024 * 1024
        ),
        name="correlate_and_regroup",
    )(
        *(
            pltpu.with_memory_space_constraint(operand, pltpu.HBM)
            for operand in (
                flat,
                window.reshape(1, FFT_LEN),
                group_of_device.reshape(1, STN),
                owner_map,
                jnp.asarray(dft_table()),
            )
        )
    )
    got = got.reshape(2, NF * CH_OUT, 8, 2, 128).transpose(0, 1, 3, 2, 4)
    return got.reshape(2, NF * CH_OUT, 1, 2, ROWS * ROWS)


def solution(mesh):
    return jax.shard_map(
        shards,
        mesh=mesh,
        in_specs=(P("freq", "stn", None, None, None), P(), P(), P()),
        out_specs=P(None, None, "stn", "freq", None),
        check_vma=False,
    )
```

```python
import math

import jax
import jax.numpy as jnp
import numpy as np
from jax import lax
from jax.experimental import pallas as pl
from jax.experimental.pallas import tpu as pltpu
from jax.sharding import PartitionSpec as P

FFT_LEN = 128
AVG = 16
SPEC = 24
CH_OUT = 8
ROWS = 32
DEPTH = 2 * SPEC * AVG
NX = 4
NZ = 8
NF = 16
STN = NX * NZ
MESH = pl.DeviceIdType.MESH
PLAN = ((0, 1), (0, 2), (0, 3), (1, 0), (1, 1), (1, 2), (1, 3))
RELAYED = 0


def dft_table():
    index = np.arange(FFT_LEN)
    theta = (index[:, None] * index[None, :] % FFT_LEN) * (2.0 * math.pi / FFT_LEN)
    table = np.concatenate([np.cos(theta), np.sin(theta)], axis=1) / math.sqrt(FFT_LEN)
    return table.astype(np.float32)


def swap_blocks(blocks, width, lane):
    blocks = list(blocks)
    step = 1
    while step < len(blocks):
        low = (lane // (width * step)) % 2 == 0
        shift = width * step
        for i in range(len(blocks)):
            if i & step:
                continue
            a, b = blocks[i], blocks[i | step]
            blocks[i] = jnp.where(low, a, pltpu.roll(b, shift, 1))
            blocks[i | step] = jnp.where(low, pltpu.roll(a, 128 - shift, 1), b)
        step *= 2
    return blocks


def column(row, size):
    lane = lax.broadcasted_iota(jnp.int32, (size, size), 1)
    sub = lax.broadcasted_iota(jnp.int32, (size, size), 0)
    return jnp.sum(jnp.where(lane == sub, row, jnp.zeros_like(row)), axis=1, keepdims=True)


def kernel(
    samples_hbm, window_hbm, groups_hbm, owners_hbm, table_hbm, out,
    samples, window, groups, owners, table, tab_vmem, tab,
    uc, us, chan, held, mixed, pairs, outgoing,
    load_sem, chunk_sem, in_send, in_recv, out_send, out_recv, own_sem, heard, crossed, known, go,
):
    f = lax.axis_index("freq")
    s = lax.axis_index("stn")
    x = s // NZ
    zl = s % NZ

    barrier = pltpu.get_barrier_semaphore()
    flip = f + 2 - 4 * ((f // 2) % 2)
    facing = x * NZ + NZ - 1 - zl
    border = jnp.logical_or(zl == 0, zl == NZ - 1)

    def signal(semaphore, to_f, to_s):
        pl.semaphore_signal(semaphore, inc=1, device_id=(to_f, to_s), device_id_type=MESH)

    for d in range(1, NZ):
        signal(barrier, f, x * NZ + (zl + d) % NZ)
    for d in range(1, NX):
        signal(barrier, f, ((x + d) % NX) * NZ + zl)
    for d in range(1, NF // 2):
        y_core = (f // 4 * 2 + f % 2 + d) % (NF // 2)
        signal(barrier, y_core // 2 * 4 + f // 2 % 2 * 2 + y_core % 2, s)

    @pl.when(border)
    def _():
        signal(barrier, flip, facing)

    loads = [
        pltpu.make_async_copy(src, dst, load_sem.at[n])
        for n, (src, dst) in enumerate(
            [(window_hbm, window), (table_hbm, table), (groups_hbm, groups), (owners_hbm, owners)]
        )
    ]
    chunk = 256
    chunks = 2 * ROWS * SPEC // chunk

    def load_chunk(i):
        rows = pl.ds(pl.multiple_of(i * chunk, chunk), chunk)
        return pltpu.make_async_copy(
            samples_hbm.at[rows, :], samples.at[rows, :], chunk_sem.at[i]
        )

    loads[0].start()
    loads[1].start()
    for i in range(chunks):
        load_chunk(i).start()
    loads[2].start()
    loads[3].start()

    loads[0].wait()
    loads[1].wait()
    taps = table[...] * column(window[...], FFT_LEN)
    high = taps.astype(jnp.bfloat16)
    low = (taps - high.astype(jnp.float32)).astype(jnp.bfloat16)
    both = jnp.concatenate([high, low], axis=0)

    @pl.loop(0, chunks)
    def _(i):
        rows = pl.ds(pl.multiple_of(i * chunk, chunk), chunk)
        load_chunk(i).wait()
        block = samples[rows, :]
        full = jnp.dot(
            jnp.concatenate([block, block], axis=1), both, preferred_element_type=jnp.float32
        )
        uc[rows, :] = full[:, :FFT_LEN]
        us[rows, :] = full[:, FFT_LEN:]

    lane = lax.broadcasted_iota(jnp.int32, (ROWS, 128), 1)
    for t8 in range(SPEC // 8):
        for part in range(2):
            blocks = []
            for t in range(8):
                at = 2 * (t8 * 8 + t)
                re = pl.ds(at, ROWS, stride=2 * SPEC)
                im = pl.ds(at + 1, ROWS, stride=2 * SPEC)
                if part == 0:
                    blocks.append(uc[re, :] + us[im, :])
                else:
                    blocks.append(uc[im, :] - us[re, :])
            blocks = swap_blocks(blocks, AVG, lane)
            for k in range(CH_OUT):
                start = (2 * t8 + part) * 128
                chan[k, :, start : start + 128] = blocks[k].astype(jnp.bfloat16)
    held[s] = chan[zl]

    @pl.when(border)
    def _():
        pl.semaphore_wait(barrier, NZ + NX + NF // 2 - 2)

    @pl.when(jnp.logical_not(border))
    def _():
        pl.semaphore_wait(barrier, NZ + NX + NF // 2 - 3)

    @pl.when(zl != NZ - 1)
    def _():
        signal(heard, f, x * NZ + NZ - 1)


    half = NZ // 2

    def turn(n):
        other, step = PLAN[n]
        high = (zl // 2 + step // 2) % 2
        low = (zl + step) % 2
        return (zl // half + other) % 2 * half + high * 2 + low

    def block_to(src, at, to_x, to_z):
        return pltpu.make_async_remote_copy(
            src_ref=src,
            dst_ref=held.at[at],
            send_sem=in_send,
            recv_sem=in_recv.at[at],
            device_id=(f, to_x * NZ + to_z),
            device_id_type=MESH,
        )

    right = (x + 1) % NX
    left = (x + 3) % NX

    def forward(at, to_x):
        block_to(held.at[at], at, to_x, zl).start()

    def place_of(of_x, n):
        return of_x * NZ + (turn(n) if n >= 0 else zl)

    def share(n):
        at = place_of(x, n)
        if n + 1 >= RELAYED:
            forward(at, (x + 2) % NX)
        forward(at, right if n % 2 else left)
        forward(at, left if n % 2 else right)

    def arrived(at):
        block_to(held.at[at], at, right, zl).wait_recv()

    def relay(n):
        came, to_x = (left, right) if n % 2 else (right, left)
        at = place_of(came, n)
        arrived(at)
        forward(at, to_x)

    second = 1 - f % 2

    @pl.when(second == 0)
    def _():
        for n in range(NZ - 1):
            to = turn(n)
            block_to(chan.at[to], s, x, to).start()

    share(-1)

    loads[2].wait()
    loads[3].wait()
    wide = lax.broadcasted_iota(jnp.int32, (STN, STN), 1)
    tall = lax.broadcasted_iota(jnp.int32, (STN, STN), 0)
    group_row = groups[...]
    row_source = jnp.max(jnp.where(group_row == tall, wide, 0), axis=1, keepdims=True)
    source_row = jnp.max(
        jnp.where(column(group_row, STN) == wide, tall, 0), axis=0, keepdims=True
    )
    place = lax.broadcasted_iota(jnp.int32, (STN, 128), 1)
    sources = jnp.where(place == NZ, row_source, 0)
    for oz in range(NZ):
        picked = jnp.where(owners[...] == x * NZ + oz, source_row, 0)
        sources = jnp.where(place == oz, jnp.max(picked, axis=1, keepdims=True), sources)
    tab_vmem[...] = sources
    to_scalars = pltpu.make_async_copy(tab_vmem, tab, load_sem.at[0])
    to_scalars.start()
    to_scalars.wait()

    @pl.when(second == 1)
    def _():
        pl.semaphore_wait(go, 1)
        for n in range(NZ - 1):
            to = turn(n)
            block_to(chan.at[to], s, x, to).start()

    for n in range(NZ - 1):
        arrived(place_of(x, n))
        share(n)
        if n - 2 >= -1 and n - 1 < RELAYED:
            relay(n - 2)
        if n == 5:

            @pl.when(second == 0)
            def _():
                signal(go, f - 1, s)

        if n == 3:

            @pl.when(zl == NZ - 1)
            def _():
                pl.semaphore_wait(heard, NZ - 1)
                signal(crossed, flip, facing)

        if n == 5:

            @pl.when(zl == 0)
            def _():
                pl.semaphore_wait(crossed, 1)
                for z in range(1, NZ):
                    signal(known, f, x * NZ + z)

    for n in range(-1, NZ - 1):
        if n + 1 < RELAYED:
            arrived(place_of(right if n % 2 else left, n))
        else:
            arrived(place_of(left, n))
            arrived(place_of(right, n))
        arrived(place_of((x + 2) % NX, n))

    @pl.when(zl != 0)
    def _():
        pl.semaphore_wait(known, 1)

    lane8 = lax.broadcasted_iota(jnp.int32, (8, 128), 1)
    channel = f * CH_OUT + zl

    @pl.loop(0, NF)
    def _(i):
        y_core = (f // 4 * 2 + f % 2 + jnp.where(second == 0, i // 2, i)) % (NF // 2)
        p = y_core // 2 * 4 + (f // 2 + 1 + jnp.where(second == 0, i, i // (NF // 2))) % 2 * 2 + y_core % 2
        for r in range(2):
            g1 = 2 * p + r
            a = held[tab[g1, NZ]]
            turned = []
            for t8 in range(SPEC // 8):
                turned.append(a[:, (2 * t8 + 1) * 128 : (2 * t8 + 2) * 128])
                turned.append(-a[:, 2 * t8 * 128 : (2 * t8 + 1) * 128])
            left = jnp.concatenate([a, jnp.concatenate(turned, axis=1)], axis=0)
            right = jnp.concatenate(
                [held[tab[g1, oz]] for oz in range(NZ)], axis=0
            )
            vis = lax.dot_general(
                left, right, (((1,), (1,)), ((), ())), preferred_element_type=jnp.float32
            ) * (1.0 / (AVG * SPEC))
            for h in range(2):
                mixed[r, h] = vis[:, h * 128 : (h + 1) * 128]
                for part in range(2):
                    blocks = [
                        mixed[r, h, pl.ds(part * ROWS + j, 8, stride=4), :] for j in range(4)
                    ]
                    blocks = swap_blocks(blocks, ROWS, lane8)
                    for q in range(4):
                        pairs[4 * h + q, part, pl.ds(r, 8, stride=2), :] = blocks[q]
        outgoing[i] = pairs[...].astype(jnp.bfloat16)
        for d in range(NZ):
            oz = (zl + d) % NZ
            mine = jnp.logical_and(p == f, d == 0)

            @pl.when(jnp.logical_not(mine))
            def _():
                pltpu.make_async_remote_copy(
                    src_ref=outgoing.at[i, oz],
                    dst_ref=out.at[:, channel],
                    send_sem=out_send,
                    recv_sem=out_recv,
                    device_id=(p, x * NZ + oz),
                    device_id_type=MESH,
                ).start()

            @pl.when(mine)
            def _():
                pltpu.make_async_copy(
                    outgoing.at[i, oz], out.at[:, channel], own_sem
                ).start()

    pltpu.make_async_copy(outgoing.at[0, 0], out.at[:, channel], own_sem).wait()
    rest = pltpu.make_async_remote_copy(
        src_ref=out.at[:, pl.ds(0, NF * NZ - 1)],
        dst_ref=out.at[:, pl.ds(0, NF * NZ - 1)],
        send_sem=out_send,
        recv_sem=out_recv,
        device_id=(f, x * NZ + (zl + 1) % NZ),
        device_id_type=MESH,
    )
    rest.wait_send()
    rest.wait_recv()
    sent = pltpu.make_async_remote_copy(
        src_ref=held.at[pl.ds(0, STN - 1)],
        dst_ref=held.at[pl.ds(0, STN - 1)],
        send_sem=in_send,
        recv_sem=in_recv.at[0],
        device_id=(f, x * NZ + (zl + 1) % NZ),
        device_id_type=MESH,
    )
    sent.wait_send()


def shards(samples, window, group_of_device, owner_map):
    flat = samples.reshape(2 * ROWS * SPEC, FFT_LEN)
    hbm = pl.BlockSpec(memory_space=pltpu.HBM)
    got = pl.pallas_call(
        kernel,
        out_shape=jax.ShapeDtypeStruct((2, NF * CH_OUT, 16, 128), jnp.bfloat16),
        in_specs=[hbm] * 5,
        out_specs=pl.BlockSpec(memory_space=pl.ANY),
        scratch_shapes=[
            pltpu.VMEM((2 * ROWS * SPEC, FFT_LEN), jnp.bfloat16),
            pltpu.VMEM((1, FFT_LEN), jnp.float32),
            pltpu.VMEM((1, STN), jnp.int32),
            pltpu.VMEM((STN, STN), jnp.int32),
            pltpu.VMEM((FFT_LEN, 2 * FFT_LEN), jnp.float32),
            pltpu.VMEM((STN, 128), jnp.int32),
            pltpu.SMEM((STN, 128), jnp.int32),
            pltpu.VMEM((2 * ROWS * SPEC, FFT_LEN), jnp.float32),
            pltpu.VMEM((2 * ROWS * SPEC, FFT_LEN), jnp.float32),
            pltpu.VMEM((CH_OUT, ROWS, DEPTH), jnp.bfloat16),
            pltpu.VMEM((STN, ROWS, DEPTH), jnp.bfloat16),
            pltpu.VMEM((2, 2, 2 * ROWS, 128), jnp.float32),
            pltpu.VMEM((NZ, 2, 16, 128), jnp.float32),
            pltpu.VMEM((NF, NZ, 2, 16, 128), jnp.bfloat16),
            pltpu.SemaphoreType.DMA((4,)),
            pltpu.SemaphoreType.DMA((6,)),
            pltpu.SemaphoreType.DMA,
            pltpu.SemaphoreType.DMA((STN,)),
            pltpu.SemaphoreType.DMA,
            pltpu.SemaphoreType.DMA,
            pltpu.SemaphoreType.DMA,
            pltpu.SemaphoreType.REGULAR,
            pltpu.SemaphoreType.REGULAR,
            pltpu.SemaphoreType.REGULAR,
            pltpu.SemaphoreType.REGULAR,
        ],
        compiler_params=pltpu.CompilerParams(
            has_side_effects=True, collective_id=0, vmem_limit_bytes=32 * 1024 * 1024
        ),
        name="correlate_and_regroup",
    )(
        *(
            pltpu.with_memory_space_constraint(operand, pltpu.HBM)
            for operand in (
                flat,
                window.reshape(1, FFT_LEN),
                group_of_device.reshape(1, STN),
                owner_map,
                jnp.asarray(dft_table()),
            )
        )
    )
    got = got.reshape(2, NF * CH_OUT, 8, 2, 128).transpose(0, 1, 3, 2, 4)
    return got.reshape(2, NF * CH_OUT, 1, 2, ROWS * ROWS)


def solution(mesh):
    return jax.shard_map(
        shards,
        mesh=mesh,
        in_specs=(P("freq", "stn", None, None, None), P(), P(), P()),
        out_specs=P(None, None, "stn", "freq", None),
        check_vma=False,
    )
```
